32 devices in a mesh: rows: 8 (over z, y), grp: 4 (over x, core).
Axes of the slice: x: 2, y: 2, z: 4, core: 2. Of those that a mesh axis runs over, the one named last changes fastest.
Arguments:
- hamiltonian: float32 [13824, 13824], P(('rows', 'grp')), as said below
- current: float32 [13824, 16], P(('rows', 'grp')), may hold values from -6 to 6
- previous: float32 [13824, 16], P(('rows', 'grp')), may hold values from -6 to 6
Outputs:
- new_current: float32 [13824, 16], P(('rows', 'grp'))
- new_previous: float32 [13824, 16], P(('rows', 'grp'))
- residual_rms: float32 [16], replicated
The draws below stay inside these ranges and needn't reach their ends.
Inputs may be any that keep to these rules, and one draw needn't show every extreme that they name: hamiltonian is symmetric: hamiltonian[i, j] equals hamiltonian[j, i].
All inputs are finite; a program needn't handle non-finite values.
Results may differ from the reference program's by a relative error of at most 0.0003.
Values sent between devices are 32-bit elements; how exact they have to be, the bound alone decides.
A program may use at most 64 MiB of HBM per device.

```python
import math
import jax
import jax.numpy as jnp
from jax import lax

NEIG = 16
SIGN_STEPS = 6
ORDER = 13824


def draw_hamiltonian(key, part):
    base = jax.random.fold_in(key, 11)
    key_energy, key_kernel = jax.random.split(base)
    energy = jnp.exp(jax.random.uniform(key_energy, (ORDER,), jnp.float32, 0.0, math.log(10.0)))
    coupling = 1.0
    noise = jax.random.normal(key_kernel, (ORDER, ORDER), jnp.float32)
    kernel = (noise + noise.T) * (coupling / math.sqrt(2.0 * ORDER))
    return kernel + jnp.diag(energy)


def steps_of(rng, shape, shards, smallest, largest):
    def one(position, parts):
        draws = jax.random.uniform(jax.random.fold_in(jax.random.fold_in(rng, 6), position), (parts,), jnp.float32, smallest / len(shards), largest / len(shards))
        return jnp.repeat(jnp.exp(draws), shape[position] // parts).reshape((-1,) + (1,) * (len(shape) - position - 1))

    gain = one(*shards[0])
    for cut in shards[1:]:
        gain = gain * one(*cut)
    return gain


def scatter_about(stream_key, extent, spread, bound, shards=(), kind=jnp.bfloat16):
    values = jax.random.normal(stream_key, extent, jnp.float32) * spread
    if len(shards) > 0:
        values = steps_of(stream_key, extent, shards, -0.22, 0.18) * values
    return jnp.clip(values, min=-bound, max=bound).astype(kind)


def setup_inputs(seed: int = 0) -> dict:
    streams_of = jax.random.split(jax.random.key(seed), 4)
    hamiltonian = draw_hamiltonian(jax.random.fold_in(streams_of[3], 71), 0)
    current = scatter_about(streams_of[1], (ORDER, NEIG), 1.0, 6.0, ((0, 32),), jnp.float32)
    previous = scatter_about(streams_of[2], (ORDER, NEIG), 1.0, 6.0, ((0, 32),), jnp.float32)
    return dict(hamiltonian=hamiltonian, current=current, previous=previous)


highest = lax.Precision.HIGHEST
eps_value = 1e-06

def mat_mul(left, right):
    return jnp.dot(left.astype(jnp.float32), right.astype(jnp.float32), precision=highest, preferred_element_type=jnp.float32)

def diag_of(matrix):
    mask = jnp.eye(matrix.shape[0], dtype=matrix.dtype)
    return lax.optimization_barrier(jnp.sum(matrix * mask, axis=1))

def ritz_update(stiff, mass):
    stiff_sym = 0.5 * (stiff + stiff.T)
    lower = jnp.linalg.cholesky(mass)
    half_way = jax.scipy.linalg.solve_triangular(lower, stiff_sym, lower=True)
    reduced = jax.scipy.linalg.solve_triangular(lower, half_way.T, lower=True)
    identity = jnp.eye(reduced.shape[0], dtype=reduced.dtype)
    level = jnp.max(diag_of(reduced)[:NEIG])
    signed = level * identity - reduced
    signed = signed / jnp.sqrt(jnp.sum(signed * signed))
    for sweep_index in range(SIGN_STEPS):
        signed = 1.5 * signed - 0.5 * mat_mul(signed, mat_mul(signed, signed))
    projector = 0.5 * (identity + signed)
    coeffs = jax.scipy.linalg.solve_triangular(lower, projector[:, :NEIG], trans=1, lower=True)
    return coeffs * math.sqrt(ORDER)

def reference(hamiltonian, current, previous):
    diag_vals = diag_of(hamiltonian)
    image = mat_mul(hamiltonian, current)
    ritz = mat_mul(current.T, image) / ORDER
    resid = image - mat_mul(current, ritz)
    residual_rms = jnp.sqrt(lax.optimization_barrier(jnp.sum(resid * resid, axis=0)) / ORDER + eps_value)
    shift = jnp.maximum(jnp.abs(diag_vals[:, None] - diag_of(ritz)[None, :]), 1.0)
    search = resid / (shift * residual_rms[None, :])
    basis = jnp.concatenate([current, search, previous], axis=1)
    himage = mat_mul(hamiltonian, basis)
    stiff = mat_mul(basis.T, himage)
    mass = mat_mul(basis.T, basis)
    coeffs = ritz_update(stiff, mass)
    new_current = mat_mul(basis, coeffs)
    new_previous = mat_mul(basis[:, NEIG:], coeffs[NEIG:])
    return (new_current, new_previous, residual_rms)
```

```python
import functools
import math

import jax
import jax.numpy as jnp
from jax import lax
from jax.experimental import pallas as pl
from jax.experimental.pallas import tpu as pltpu
from jax.sharding import PartitionSpec as P

SIGN_STEPS = 6
EPS = 1e-06
MESH = pl.DeviceIdType.MESH
F32 = jnp.float32
BF16 = jnp.bfloat16
NT = (((1,), (1,)), ((), ()))
NN = (((1,), (0,)), ((), ()))


def dot_hi(a, b, dims=NN):
    return lax.dot_general(a, b, dims, precision=lax.Precision.HIGHEST, preferred_element_type=F32)


def dot_bf(a, b, dims=NN):
    return lax.dot_general(a, b, dims, preferred_element_type=F32)


def split(x):
    hi = x.astype(BF16)
    return hi, (x - hi.astype(F32)).astype(BF16)


def iota(shape, axis):
    return lax.broadcasted_iota(jnp.int32, shape, axis)


def kernel(R, G, rows, K, n, T, MW,
           h_ref, cur_ref, prev_ref, nc_ref, np_ref, rms_ref,
           hf, hhi, hlo, b1, b2, b3, b4, b5, vc, vp, vi, vbc, vbp, vbs, acc, basis, rhs, tr,
           hsem, ss, rs, fs, fr):
    half = G // 2
    C = R * half
    D = 2 * C
    W = MW + 128
    TK = K // T
    r = lax.axis_index("rows")
    g = lax.axis_index("grp")
    core = lax.rem(g, 2)
    chip = r * half + g // 2
    dev = 2 * chip + core

    def ident(q, k):
        return (q // half, lax.rem(q, half) * 2 + k)

    for t in range(T):
        cs = slice(t * TK, (t + 1) * TK)
        pltpu.make_async_copy(h_ref.at[:, cs], hf.at[:, cs], hsem.at[t]).start()

    barrier = pltpu.get_barrier_semaphore()

    def greet(p, _):
        pl.semaphore_signal(barrier, inc=1, device_id=ident(lax.rem(chip + p, C), core), device_id_type=MESH)
        return 0

    lax.fori_loop(1, C, greet, 0)
    pl.semaphore_signal(barrier, inc=1, device_id=ident(chip, 1 - core), device_id_type=MESH)
    pl.semaphore_wait(barrier, C)

    def direct(m, buf, src, p):
        return pltpu.make_async_remote_copy(
            src_ref=src, dst_ref=buf.at[dev], send_sem=ss.at[m, p], recv_sem=rs.at[m, chip],
            device_id=ident(lax.rem(chip + p, C), core), device_id_type=MESH)

    def arrive(m, buf, q):
        return pltpu.make_async_remote_copy(
            src_ref=buf.at[2 * q + core], dst_ref=buf.at[2 * q + core], send_sem=ss.at[m, 0],
            recv_sem=rs.at[m, q], device_id=ident(q, core), device_id_type=MESH)

    def forward(m, buf, q, src):
        return pltpu.make_async_remote_copy(
            src_ref=src, dst_ref=buf.at[2 * q + core], send_sem=fs.at[m, q], recv_sem=fr.at[m, q],
            device_id=ident(chip, 1 - core), device_id_type=MESH)

    def send(m, buf, src=None):
        src = buf.at[dev] if src is None else src

        def one(p, _):
            direct(m, buf, src, p).start()
            return 0

        lax.fori_loop(1, C, one, 0)
        forward(m, buf, chip, src).start()

    def relay(m, buf):
        def one(p, _):
            q = lax.rem(chip + C - p, C)
            arrive(m, buf, q).wait_recv()
            forward(m, buf, q, buf.at[2 * q + core]).start()
            return 0

        lax.fori_loop(1, C, one, 0)

    def collect(m, buf):
        def one(q, _):
            pltpu.make_async_remote_copy(
                src_ref=buf.at[2 * q + 1 - core], dst_ref=buf.at[2 * q + 1 - core], send_sem=fs.at[m, q],
                recv_sem=fr.at[m, q], device_id=ident(chip, 1 - core), device_id_type=MESH).wait_recv()
            return 0

        lax.fori_loop(0, C, one, 0)

    def drain(m, buf):
        def one(p, _):
            direct(m, buf, buf.at[dev], p).wait_send()
            return 0

        lax.fori_loop(1, C, one, 0)

        def two(q, _):
            forward(m, buf, q, buf.at[2 * q + core]).wait_send()
            return 0

        lax.fori_loop(0, C, two, 0)

    def assemble(buf, dst, masked):
        height = dst.shape[0]
        dst[...] = jnp.zeros_like(dst)
        keep = iota((height, MW), 1) < rows
        pad = jnp.zeros((height, 128), F32)
        for d in range(D):
            start = d * rows // 128 * 128
            x = buf[d]
            if masked:
                x = jnp.where(keep, x, 0.0)
            x = jnp.concatenate([x, pad], axis=1)
            shift = d * rows - start
            if shift:
                x = pltpu.roll(x, shift, 1)
            dst[:, start:start + W] += x

    def split_into(vb, v):
        hi, lo = split(v[0:n, 0:K])
        vb[0:n, :] = hi
        vb[n:2 * n, :] = lo

    def apply_ham(vb, first, last):
        def one(t, _):
            cols = pl.ds(pl.multiple_of(t * TK, 128), TK)
            v = vb[:, cols]
            acc[0:rows, 0:2 * n] += dot_bf(hhi[:, cols], v, NT) + dot_bf(hlo[:, cols], v, NT)
            return 0

        lax.fori_loop(first, last, one, 0)

    def clear():
        acc[...] = jnp.zeros_like(acc)

    def product():
        flat = acc[...].T
        return flat[0:n, :] + flat[n:2 * n, :]

    b1[dev] = cur_ref[...]
    send(0, b1, cur_ref)
    for t in range(T):
        cs = slice(t * TK, (t + 1) * TK)
        pltpu.make_async_copy(h_ref.at[:, cs], hf.at[:, cs], hsem.at[t]).wait()

        def part(s, _, t=t):
            cols = pl.ds(pl.multiple_of(t * TK + s * 128, 128), 128)
            hi, lo = split(hf[:, cols])
            hhi[:, cols] = hi
            hlo[:, cols] = lo
            return 0

        lax.fori_loop(0, TK // 128, part, 0)
    relay(0, b1)

    base = dev * rows // 128 * 128
    shift = dev * rows - base
    window = hf[:, pl.ds(pl.multiple_of(base, 128), W)]
    on_diag = iota((rows, W), 1) == iota((rows, W), 0) + shift
    own_diag = jnp.sum(jnp.where(on_diag, window, 0.0), axis=0, keepdims=True)
    own_diag = pltpu.roll(jnp.broadcast_to(own_diag, (8, W)), lax.rem(W - shift, W), 1)[:, 0:MW]
    b2[dev, 0:n, :] = prev_ref[...]
    b2[dev, n:n + 8, :] = own_diag
    send(1, b2)

    collect(0, b1)
    assemble(b1, vc, False)
    split_into(vbc, vc)
    clear()
    apply_ham(vbc, 0, T)
    image = product()
    cur = cur_ref[...]
    prev = prev_ref[...]
    cross = dot_hi(image, cur, NT)
    wide = jnp.concatenate([jnp.zeros((n, rows), F32), cross], axis=1)
    wide = jnp.concatenate([wide, jnp.zeros((n, MW - rows - n), F32)], axis=1)
    b3[dev] = image + wide
    send(2, b3)

    relay(1, b2)
    collect(1, b2)
    assemble(b2, vp, False)
    split_into(vbp, vp)
    clear()
    cut = (2 * T) // 3
    apply_ham(vbp, 0, cut)
    relay(2, b3)
    apply_ham(vbp, cut, T)
    hprev = product()
    collect(2, b3)

    tail = jnp.zeros((n, 128), F32)
    for d in range(D):
        tail = tail + b3[d, :, MW - 128:MW]
    tail = pltpu.roll(tail, (MW - rows) % 128, 1)
    tail = jnp.where(iota((n, 128), 1) < n, tail, 0.0)
    ritz = tail / K
    ritz_diag = jnp.sum(jnp.where(iota((n, 128), 0) == iota((n, 128), 1), ritz, 0.0), axis=1, keepdims=True)
    twice_hi, twice_lo = split(ritz + pltpu.roll(ritz, n, 1))
    twice_hi = twice_hi[:, 0:2 * n]
    twice_lo = twice_lo[:, 0:2 * n]
    assemble(b3, vi, True)

    def search_part(t, total):
        cols = pl.ds(pl.multiple_of(t * TK, 128), TK)
        v = vbc[:, cols]
        resid = vi[:, cols] - (dot_bf(twice_hi, v) + dot_bf(twice_lo, v))
        shifts = jnp.maximum(jnp.abs(vp[n:n + 1, cols] - ritz_diag), 1.0)
        hi, lo = split(resid / shifts)
        vbs[0:n, cols] = hi
        vbs[n:2 * n, cols] = lo
        return total + jnp.sum(resid * resid, axis=1, keepdims=True)

    total = lax.fori_loop(0, T, search_part, jnp.zeros((n, 1), F32))
    rms = jnp.sqrt(total / K + EPS)
    rms_ref[...] = jnp.broadcast_to(rms, (n, 128))

    resid = image - dot_hi(ritz[:, 0:n], cur)
    shifts = jnp.maximum(jnp.abs(own_diag[0:1, :] - ritz_diag), 1.0)
    basis[0:n, :] = cur
    basis[n:2 * n, :] = resid / (shifts * rms)
    basis[2 * n:3 * n, :] = prev
    rhs[...] = jnp.zeros_like(rhs)
    rhs[0:n, :] = image
    rhs[2 * n:3 * n, :] = hprev
    rhs[4 * n:7 * n, :] = basis[...]
    b4[dev] = dot_hi(basis[...], rhs[...], NT)
    send(3, b4)

    clear()
    apply_ham(vbs, 0, cut)
    relay(3, b4)
    apply_ham(vbs, cut, T)
    hsearch = product() / rms
    rhs[0:3 * n, :] = basis[...]
    b5[dev] = dot_hi(hsearch, rhs[...], NT)
    send(4, b5)

    collect(3, b4)
    sums = b4[0]
    for d in range(1, D):
        sums = sums + b4[d]
    N3 = 3 * n
    row_id = iota((N3, 128), 0)
    lane_id = iota((N3, 128), 1)
    work = jnp.where(lane_id < 4 * n, pltpu.roll(sums, 4 * n, 1), 0.0)
    work = jnp.where(lane_id == row_id + 4 * n, 1.0, work)
    for k in range(N3):
        pivot_row = work[k:k + 1, :] / work[k:k + 1, k:k + 1]
        factor = jnp.where(row_id > k, work[:, k:k + 1], 0.0)
        work = work - factor * pivot_row
    pivots = jnp.sum(jnp.where(row_id == lane_id, work, 0.0), axis=1, keepdims=True)
    work = work / jnp.sqrt(pivots)
    inverse = pltpu.roll(work, 4 * n, 1)[:, 0:N3]

    relay(4, b5)
    collect(4, b5)
    last = b5[0]
    for d in range(1, D):
        last = last + b5[d]
    tr[0:128, 0:128] = jnp.zeros((128, 128), F32)
    tr[n:2 * n, 0:128] = last
    stiff = jnp.where(lane_id < N3, sums, 0.0) + tr[0:128, 0:128].T[0:N3, :]
    tr[0:128, 0:128] = jnp.zeros((128, 128), F32)
    tr[0:N3, 0:128] = stiff
    stiff = (0.5 * (stiff + tr[0:128, 0:128].T[0:N3, :]))[:, 0:N3]
    reduced = dot_hi(dot_hi(inverse, stiff), inverse, NT)
    eye = jnp.where(iota((N3, N3), 0) == iota((N3, N3), 1), 1.0, 0.0).astype(F32)
    ours = (iota((N3, N3), 0) == iota((N3, N3), 1)) & (iota((N3, N3), 0) < n)
    level = jnp.max(jnp.where(ours, reduced, -jnp.inf), keepdims=True)
    signed = level * eye - reduced
    signed = signed / jnp.sqrt(jnp.sum(signed * signed, keepdims=True))
    for _ in range(SIGN_STEPS):
        signed = 1.5 * signed - 0.5 * dot_hi(signed, dot_hi(signed, signed))
    projector = 0.5 * (eye + signed)
    coeffs = dot_hi(projector[0:n, :], inverse) * math.sqrt(K)
    nc_ref[...] = dot_hi(coeffs, basis[...])
    np_ref[...] = dot_hi(jnp.where(iota((n, N3), 1) >= n, coeffs, 0.0), basis[...])

    for m, buf in enumerate((b1, b2, b3, b4, b5)):
        drain(m, buf)


def body(R, G, hamiltonian, current, previous):
    rows, n = current.shape
    K = hamiltonian.shape[1]
    C = R * G // 2
    D = 2 * C
    T = 9
    MW = -(-(rows + n) // 128) * 128
    W = MW + 128
    TW = max(MW, 128)
    pad = ((0, 0), (0, MW - rows))
    cur_t = jnp.pad(current.T, pad)
    prev_t = jnp.pad(previous.T, pad)
    vm = pl.BlockSpec(memory_space=pltpu.VMEM)
    nc, np_, rms = pl.pallas_call(
        functools.partial(kernel, R, G, rows, K, n, T, MW),
        out_shape=[jax.ShapeDtypeStruct((n, MW), F32), jax.ShapeDtypeStruct((n, MW), F32),
                   jax.ShapeDtypeStruct((n, 128), F32)],
        in_specs=[pl.BlockSpec(memory_space=pl.ANY), vm, vm],
        out_specs=[vm, vm, vm],
        scratch_shapes=[
            pltpu.VMEM((rows, K + 128), F32),
            pltpu.VMEM((rows, K), BF16),
            pltpu.VMEM((rows, K), BF16),
            pltpu.VMEM((D, n, MW), F32),
            pltpu.VMEM((D, n + 8, MW), F32),
            pltpu.VMEM((D, n, MW), F32),
            pltpu.VMEM((D, 3 * n, 128), F32),
            pltpu.VMEM((D, n, 128), F32),
            pltpu.VMEM((n, K + 128), F32),
            pltpu.VMEM((n + 8, K + 128), F32),
            pltpu.VMEM((n, K + 128), F32),
            pltpu.VMEM((2 * n, K), BF16),
            pltpu.VMEM((2 * n, K), BF16),
            pltpu.VMEM((2 * n, K), BF16),
            pltpu.VMEM((MW, 128), F32),
            pltpu.VMEM((3 * n, MW), F32),
            pltpu.VMEM((128, MW), F32),
            pltpu.VMEM((128, TW), F32),
            pltpu.SemaphoreType.DMA((T,)),
            pltpu.SemaphoreType.DMA((5, C)),
            pltpu.SemaphoreType.DMA((5, C)),
            pltpu.SemaphoreType.DMA((5, C)),
            pltpu.SemaphoreType.DMA((5, C)),
        ],
        compiler_params=pltpu.CompilerParams(
            collective_id=0, has_side_effects=True, vmem_limit_bytes=64000000),
    )(hamiltonian, cur_t, prev_t)
    return nc[:, :rows].T, np_[:, :rows].T, rms[:, 0]


def solution(mesh):
    R, G = mesh.shape["rows"], mesh.shape["grp"]
    spec = P(("rows", "grp"), None)
    return jax.shard_map(
        functools.partial(body, R, G),
        mesh=mesh,
        in_specs=(spec, spec, spec),
        out_specs=(spec, spec, P()),
        check_vma=False,
    )
```

```python
import functools
import math

import jax
import jax.numpy as jnp
from jax import lax
from jax.experimental import pallas as pl
from jax.experimental.pallas import tpu as pltpu
from jax.sharding import PartitionSpec as P

SIGN_STEPS = 6
EPS = 1e-06
MESH = pl.DeviceIdType.MESH
F32 = jnp.float32
BF16 = jnp.bfloat16
NT = (((1,), (1,)), ((), ()))
NN = (((1,), (0,)), ((), ()))


def dot_hi(a, b, dims=NN):
    return lax.dot_general(a, b, dims, precision=lax.Precision.HIGHEST, preferred_element_type=F32)


def dot_bf(a, b, dims=NN):
    return lax.dot_general(a, b, dims, preferred_element_type=F32)


def split(x):
    hi = x.astype(BF16)
    return hi, (x - hi.astype(F32)).astype(BF16)


def iota(shape, axis):
    return lax.broadcasted_iota(jnp.int32, shape, axis)


def kernel(R, G, rows, K, n, T, MW,
           h_ref, cur_ref, prev_ref, nc_ref, np_ref, rms_ref,
           hf, hhi, hlo, b1, b2, b3, b4, b5, vc, vp, vi, vbc, vbp, vbs, acc, basis, rhs, tr,
           hsem, ss, rs, fs, fr):
    half = G // 2
    C = R * half
    D = 2 * C
    W = MW + 128
    TK = K // T
    r = lax.axis_index("rows")
    g = lax.axis_index("grp")
    core = lax.rem(g, 2)
    chip = r * half + g // 2
    dev = 2 * chip + core

    def ident(q, k):
        return (q // half, lax.rem(q, half) * 2 + k)

    for t in range(T):
        cs = slice(t * TK, (t + 1) * TK)
        pltpu.make_async_copy(h_ref.at[:, cs], hf.at[:, cs], hsem.at[t]).start()

    barrier = pltpu.get_barrier_semaphore()

    def greet(p, _):
        pl.semaphore_signal(barrier, inc=1, device_id=ident(lax.rem(chip + p, C), core), device_id_type=MESH)
        return 0

    lax.fori_loop(1, C, greet, 0)
    pl.semaphore_signal(barrier, inc=1, device_id=ident(chip, 1 - core), device_id_type=MESH)
    pl.semaphore_wait(barrier, C)

    def direct(m, buf, src, p):
        return pltpu.make_async_remote_copy(
            src_ref=src, dst_ref=buf.at[dev], send_sem=ss.at[m, p], recv_sem=rs.at[m, chip],
            device_id=ident(lax.rem(chip + p, C), core), device_id_type=MESH)

    def arrive(m, buf, q):
        return pltpu.make_async_remote_copy(
            src_ref=buf.at[2 * q + core], dst_ref=buf.at[2 * q + core], send_sem=ss.at[m, 0],
            recv_sem=rs.at[m, q], device_id=ident(q, core), device_id_type=MESH)

    def forward(m, buf, q, src):
        return pltpu.make_async_remote_copy(
            src_ref=src, dst_ref=buf.at[2 * q + core], send_sem=fs.at[m, q], recv_sem=fr.at[m, q],
            device_id=ident(chip, 1 - core), device_id_type=MESH)

    def send(m, buf, src=None):
        src = buf.at[dev] if src is None else src

        def one(p, _):
            direct(m, buf, src, p).start()
            return 0

        lax.fori_loop(1, C, one, 0)
        forward(m, buf, chip, src).start()

    def relay(m, buf):
        def one(p, _):
            q = lax.rem(chip + C - p, C)
            arrive(m, buf, q).wait_recv()
            forward(m, buf, q, buf.at[2 * q + core]).start()
            return 0

        lax.fori_loop(1, C, one, 0)

    def collect(m, buf):
        def one(q, _):
            pltpu.make_async_remote_copy(
                src_ref=buf.at[2 * q + 1 - core], dst_ref=buf.at[2 * q + 1 - core], send_sem=fs.at[m, q],
                recv_sem=fr.at[m, q], device_id=ident(chip, 1 - core), device_id_type=MESH).wait_recv()
            return 0

        lax.fori_loop(0, C, one, 0)

    def drain(m, buf):
        def one(p, _):
            direct(m, buf, buf.at[dev], p).wait_send()
            return 0

        lax.fori_loop(1, C, one, 0)

        def two(q, _):
            forward(m, buf, q, buf.at[2 * q + core]).wait_send()
            return 0

        lax.fori_loop(0, C, two, 0)

    def assemble(buf, dst, masked):
        height = dst.shape[0]
        dst[...] = jnp.zeros_like(dst)
        keep = iota((height, MW), 1) < rows
        pad = jnp.zeros((height, 128), F32)
        for d in range(D):
            start = d * rows // 128 * 128
            x = buf[d]
            if masked:
                x = jnp.where(keep, x, 0.0)
            x = jnp.concatenate([x, pad], axis=1)
            shift = d * rows - start
            if shift:
                x = pltpu.roll(x, shift, 1)
            dst[:, start:start + W] += x

    def split_into(vb, v):
        hi, lo = split(v[0:n, 0:K])
        vb[0:n, :] = hi
        vb[n:2 * n, :] = lo

    def apply_ham(vb, first, last):
        def one(t, _):
            cols = pl.ds(pl.multiple_of(t * TK, 128), TK)
            v = vb[:, cols]
            acc[:, 0:rows] += dot_bf(v, hhi[:, cols], NT) + dot_bf(v, hlo[:, cols], NT)
            return 0

        lax.fori_loop(first, last, one, 0)

    def clear():
        acc[...] = jnp.zeros_like(acc)

    def product():
        return acc[0:n, :] + acc[n:2 * n, :]

    b1[dev] = cur_ref[...]
    send(0, b1, cur_ref)
    for t in range(T):
        cs = slice(t * TK, (t + 1) * TK)
        pltpu.make_async_copy(h_ref.at[:, cs], hf.at[:, cs], hsem.at[t]).wait()

        def part(s, _, t=t):
            cols = pl.ds(pl.multiple_of(t * TK + s * 128, 128), 128)
            hi, lo = split(hf[:, cols])
            hhi[:, cols] = hi
            hlo[:, cols] = lo
            return 0

        lax.fori_loop(0, TK // 128, part, 0)
    relay(0, b1)

    base = dev * rows // 128 * 128
    shift = dev * rows - base
    window = hf[:, pl.ds(pl.multiple_of(base, 128), W)]
    on_diag = iota((rows, W), 1) == iota((rows, W), 0) + shift
    own_diag = jnp.sum(jnp.where(on_diag, window, 0.0), axis=0, keepdims=True)
    own_diag = pltpu.roll(jnp.broadcast_to(own_diag, (8, W)), lax.rem(W - shift, W), 1)[:, 0:MW]
    b2[dev, 0:n, :] = prev_ref[...]
    b2[dev, n:n + 8, :] = own_diag
    send(1, b2)

    collect(0, b1)
    assemble(b1, vc, False)
    split_into(vbc, vc)
    clear()
    apply_ham(vbc, 0, T)
    image = product()
    cur = cur_ref[...]
    prev = prev_ref[...]
    cross = dot_hi(image, cur, NT)
    wide = jnp.concatenate([jnp.zeros((n, rows), F32), cross], axis=1)
    wide = jnp.concatenate([wide, jnp.zeros((n, MW - rows - n), F32)], axis=1)
    b3[dev] = image + wide
    send(2, b3)

    relay(1, b2)
    collect(1, b2)
    assemble(b2, vp, False)
    split_into(vbp, vp)
    clear()
    cut = (2 * T) // 3
    apply_ham(vbp, 0, cut)
    relay(2, b3)
    apply_ham(vbp, cut, T)
    hprev = product()
    collect(2, b3)

    tail = jnp.zeros((n, 128), F32)
    for d in range(D):
        tail = tail + b3[d, :, MW - 128:MW]
    tail = pltpu.roll(tail, (MW - rows) % 128, 1)
    tail = jnp.where(iota((n, 128), 1) < n, tail, 0.0)
    ritz = tail / K
    ritz_diag = jnp.sum(jnp.where(iota((n, 128), 0) == iota((n, 128), 1), ritz, 0.0), axis=1, keepdims=True)
    twice_hi, twice_lo = split(ritz + pltpu.roll(ritz, n, 1))
    twice_hi = twice_hi[:, 0:2 * n]
    twice_lo = twice_lo[:, 0:2 * n]
    assemble(b3, vi, True)

    def search_part(t, total):
        cols = pl.ds(pl.multiple_of(t * TK, 128), TK)
        v = vbc[:, cols]
        resid = vi[:, cols] - (dot_bf(twice_hi, v) + dot_bf(twice_lo, v))
        shifts = jnp.maximum(jnp.abs(vp[n:n + 1, cols] - ritz_diag), 1.0)
        hi, lo = split(resid / shifts)
        vbs[0:n, cols] = hi
        vbs[n:2 * n, cols] = lo
        return total + jnp.sum(resid * resid, axis=1, keepdims=True)

    total = lax.fori_loop(0, T, search_part, jnp.zeros((n, 1), F32))
    rms = jnp.sqrt(total / K + EPS)
    rms_ref[...] = jnp.broadcast_to(rms, (n, 128))

    resid = image - dot_hi(ritz[:, 0:n], cur)
    shifts = jnp.maximum(jnp.abs(own_diag[0:1, :] - ritz_diag), 1.0)
    basis[0:n, :] = cur
    basis[n:2 * n, :] = resid / (shifts * rms)
    basis[2 * n:3 * n, :] = prev
    rhs[...] = jnp.zeros_like(rhs)
    rhs[0:n, :] = image
    rhs[2 * n:3 * n, :] = hprev
    rhs[4 * n:7 * n, :] = basis[...]
    b4[dev] = dot_hi(basis[...], rhs[...], NT)
    send(3, b4)

    clear()
    apply_ham(vbs, 0, cut)
    relay(3, b4)
    apply_ham(vbs, cut, T)
    hsearch = product() / rms
    rhs[0:3 * n, :] = basis[...]
    b5[dev] = dot_hi(hsearch, rhs[...], NT)
    send(4, b5)

    collect(3, b4)
    sums = b4[0]
    for d in range(1, D):
        sums = sums + b4[d]
    N3 = 3 * n
    row_id = iota((N3, 128), 0)
    lane_id = iota((N3, 128), 1)
    work = jnp.where(lane_id < 4 * n, pltpu.roll(sums, 4 * n, 1), 0.0)
    work = jnp.where(lane_id == row_id + 4 * n, 1.0, work)
    for k in range(N3):
        pivot_row = work[k:k + 1, :] / work[k:k + 1, k:k + 1]
        factor = jnp.where(row_id > k, work[:, k:k + 1], 0.0)
        work = work - factor * pivot_row
    pivots = jnp.sum(jnp.where(row_id == lane_id, work, 0.0), axis=1, keepdims=True)
    work = work / jnp.sqrt(pivots)
    inverse = pltpu.roll(work, 4 * n, 1)[:, 0:N3]

    relay(4, b5)
    collect(4, b5)
    last = b5[0]
    for d in range(1, D):
        last = last + b5[d]
    tr[0:128, 0:128] = jnp.zeros((128, 128), F32)
    tr[n:2 * n, 0:128] = last
    stiff = jnp.where(lane_id < N3, sums, 0.0) + tr[0:128, 0:128].T[0:N3, :]
    tr[0:128, 0:128] = jnp.zeros((128, 128), F32)
    tr[0:N3, 0:128] = stiff
    stiff = (0.5 * (stiff + tr[0:128, 0:128].T[0:N3, :]))[:, 0:N3]
    reduced = dot_hi(dot_hi(inverse, stiff), inverse, NT)
    eye = jnp.where(iota((N3, N3), 0) == iota((N3, N3), 1), 1.0, 0.0).astype(F32)
    ours = (iota((N3, N3), 0) == iota((N3, N3), 1)) & (iota((N3, N3), 0) < n)
    level = jnp.max(jnp.where(ours, reduced, -jnp.inf), keepdims=True)
    signed = level * eye - reduced
    signed = signed / jnp.sqrt(jnp.sum(signed * signed, keepdims=True))
    for _ in range(SIGN_STEPS):
        signed = 1.5 * signed - 0.5 * dot_hi(signed, dot_hi(signed, signed))
    projector = 0.5 * (eye + signed)
    coeffs = dot_hi(projector[0:n, :], inverse) * math.sqrt(K)
    nc_ref[...] = dot_hi(coeffs, basis[...])
    np_ref[...] = dot_hi(jnp.where(iota((n, N3), 1) >= n, coeffs, 0.0), basis[...])

    for m, buf in enumerate((b1, b2, b3, b4, b5)):
        drain(m, buf)


def body(R, G, hamiltonian, current, previous):
    rows, n = current.shape
    K = hamiltonian.shape[1]
    C = R * G // 2
    D = 2 * C
    T = 9
    MW = -(-(rows + n) // 128) * 128
    W = MW + 128
    TW = max(MW, 128)
    pad = ((0, 0), (0, MW - rows))
    cur_t = jnp.pad(current.T, pad)
    prev_t = jnp.pad(previous.T, pad)
    vm = pl.BlockSpec(memory_space=pltpu.VMEM)
    nc, np_, rms = pl.pallas_call(
        functools.partial(kernel, R, G, rows, K, n, T, MW),
        out_shape=[jax.ShapeDtypeStruct((n, MW), F32), jax.ShapeDtypeStruct((n, MW), F32),
                   jax.ShapeDtypeStruct((n, 128), F32)],
        in_specs=[pl.BlockSpec(memory_space=pl.ANY), vm, vm],
        out_specs=[vm, vm, vm],
        scratch_shapes=[
            pltpu.VMEM((rows, K + 128), F32),
            pltpu.VMEM((rows, K), BF16),
            pltpu.VMEM((rows, K), BF16),
            pltpu.VMEM((D, n, MW), F32),
            pltpu.VMEM((D, n + 8, MW), F32),
            pltpu.VMEM((D, n, MW), F32),
            pltpu.VMEM((D, 3 * n, 128), F32),
            pltpu.VMEM((D, n, 128), F32),
            pltpu.VMEM((n, K + 128), F32),
            pltpu.VMEM((n + 8, K + 128), F32),
            pltpu.VMEM((n, K + 128), F32),
            pltpu.VMEM((2 * n, K), BF16),
            pltpu.VMEM((2 * n, K), BF16),
            pltpu.VMEM((2 * n, K), BF16),
            pltpu.VMEM((2 * n, MW), F32),
            pltpu.VMEM((3 * n, MW), F32),
            pltpu.VMEM((128, MW), F32),
            pltpu.VMEM((128, TW), F32),
            pltpu.SemaphoreType.DMA((T,)),
            pltpu.SemaphoreType.DMA((5, C)),
            pltpu.SemaphoreType.DMA((5, C)),
            pltpu.SemaphoreType.DMA((5, C)),
            pltpu.SemaphoreType.DMA((5, C)),
        ],
        compiler_params=pltpu.CompilerParams(
            collective_id=0, has_side_effects=True, vmem_limit_bytes=64000000),
    )(hamiltonian, cur_t, prev_t)
    return nc[:, :rows].T, np_[:, :rows].T, rms[:, 0]


def solution(mesh):
    R, G = mesh.shape["rows"], mesh.shape["grp"]
    spec = P(("rows", "grp"), None)
    return jax.shard_map(
        functools.partial(body, R, G),
        mesh=mesh,
        in_specs=(spec, spec, spec),
        out_specs=(spec, spec, P()),
        check_vma=False,
    )
```
